32 devices in a mesh: section: 8 (over y, x, core), dp: 4 (over z).
Axes of the slice: x: 2, y: 2, z: 4, core: 2. Of those that a mesh axis runs over, the one named last changes fastest.
Arguments:
- out_pair: float32 [512, 2048], P('dp'), may hold values from -6 to 6
- out_grad: bfloat16 [512, 2048], P('dp'), may hold values from -6 to 6
- f_weight: bfloat16 [8, 1024, 1024], P('section', 'dp'), may hold values from -0.09375 to 0.09375
- g_weight: bfloat16 [8, 1024, 1024], P('section', 'dp'), may hold values from -0.09375 to 0.09375
- gains: float32 [8, 2, 1024], P('section'), may hold values from 0.1 to 1.9
Outputs:
- in_pair: float32 [8, 512, 2048], P('section', 'dp')
- in_grad: bfloat16 [8, 512, 2048], P('section', 'dp')
- f_grad: float32 [8, 1024, 1024], P('section', 'dp')
- g_grad: float32 [8, 1024, 1024], P('section', 'dp')
- gains_grad: float32 [8, 2, 1024], P('section')
The draws below stay inside these ranges and needn't reach their ends.
All inputs are finite; a program needn't handle non-finite values.
Results may differ from the reference program's by a relative error of at most 0.04.
Values may be sent and summed in bfloat16 or wider, within the bound.
A program may use at most 64 MiB of HBM per device.

```python
import jax
import jax.numpy as jnp
from jax import lax

DH = 1024
TOK_DEV = 128
SECTIONS = 8
TOKENS = 512
N_SECTION = 8
N_DP = 4


def steps_of(key, extent, shards, smallest, top_value):
    gain, own = 1.0, jax.random.fold_in(key, 6)
    for dim, parts in shards:
        steps = jnp.exp(jax.random.uniform(jax.random.fold_in(own, dim), (parts,), jnp.float32, smallest / len(shards), top_value / len(shards)))
        gain = gain * jnp.repeat(steps, extent[dim] // parts).reshape([-1 if axis == dim else 1 for axis in range(len(extent))])
    return gain


def centred(key, dims, width, reach, shards=(), kind=jnp.bfloat16):
    result = width * jax.random.normal(key, dims, jnp.float32)
    if shards:
        result = result * steps_of(key, dims, shards, -0.22, 0.18)
    return jnp.clip(result, -reach, reach).astype(kind)


def setup_inputs(seed: int = 0) -> dict:
    seeds = jax.random.split(jax.random.key(seed), 6)
    out_pair = centred(seeds[0], (TOKENS, 2 * DH), 1.0, 6.0, ((0, 4),), jnp.float32)
    out_grad = centred(seeds[1], (TOKENS, 2 * DH), 1.0, 6.0, ((0, 4),))
    f_weight = centred(seeds[2], (SECTIONS, DH, DH), (4 * DH) ** -0.5, 0.09375, ((0, 8), (1, 4)))
    g_weight = centred(seeds[3], (SECTIONS, DH, DH), (4 * DH) ** -0.5, 0.09375, ((0, 8), (1, 4)))
    gains = jnp.clip(1.0 + 0.18 * jax.random.normal(seeds[4], (SECTIONS, 2, DH), jnp.float32), 0.1, 1.9)
    return {"out_pair": out_pair, "out_grad": out_grad, "f_weight": f_weight, "g_weight": g_weight, "gains": gains}


offset = 0.25

def silu_parts(pre_values):
    sigmoid_value = jax.nn.sigmoid(pre_values)
    return (pre_values * sigmoid_value, sigmoid_value * (1.0 + pre_values * (1.0 - sigmoid_value)))

def normalize(values, gain_row):
    inv_scale = lax.rsqrt(lax.optimization_barrier(jnp.mean(values * values, axis=-1, keepdims=True)) + offset)
    return ((values * inv_scale * gain_row).astype(jnp.bfloat16), inv_scale)

def norm_back(values, inv_scale, gain_row, upstream):
    weighted = gain_row * upstream
    cubed = inv_scale * inv_scale * inv_scale
    return inv_scale * weighted - values * cubed * lax.optimization_barrier(jnp.mean(weighted * values, axis=-1, keepdims=True))

def coupling_back(upper_out, lower_out, upper_grad, lower_grad, w_first, w_second, gain_pair):
    normed_second, scale_second = normalize(upper_out, gain_pair[1])
    pre_second = jnp.dot(normed_second, w_second, preferred_element_type=jnp.float32)
    act_second, slope_second = silu_parts(pre_second)
    lower_in = lower_out - act_second
    normed_first, scale_first = normalize(lower_in, gain_pair[0])
    pre_first = jnp.dot(normed_first, w_first, preferred_element_type=jnp.float32)
    act_first, slope_first = silu_parts(pre_first)
    upper_in = upper_out - act_first
    delta_second = (lower_grad * slope_second).astype(jnp.bfloat16)
    back_second = jnp.dot(delta_second, w_second.T, preferred_element_type=jnp.float32)
    through = upper_grad + norm_back(upper_out, scale_second, gain_pair[1], back_second)
    delta_first = (through * slope_first).astype(jnp.bfloat16)
    back_first = jnp.dot(delta_first, w_first.T, preferred_element_type=jnp.float32)
    lower_total = lower_grad + norm_back(lower_in, scale_first, gain_pair[0], back_first)
    gain_terms = jnp.stack([lax.optimization_barrier(jnp.sum(back_first * lower_in * scale_first, axis=0)), lax.optimization_barrier(jnp.sum(back_second * upper_out * scale_second, axis=0))])
    return (upper_in, lower_in, through.astype(jnp.bfloat16), lower_total.astype(jnp.bfloat16), normed_first, delta_first, normed_second, delta_second, gain_terms)

def replica_sum(normed, delta):
    left_side = normed.reshape(N_DP, TOK_DEV, -1).astype(jnp.float32)
    right_side = delta.reshape(N_DP, TOK_DEV, -1).astype(jnp.float32)
    partial_sums = jnp.einsum('rtd,rte->rde', left_side, right_side)
    rounded = lax.optimization_barrier(partial_sums.astype(jnp.bfloat16))
    return lax.optimization_barrier(jnp.sum(rounded.astype(jnp.float32), axis=0))

def reference(out_pair, out_grad, f_weight, g_weight, gains):
    channels = out_pair.shape[1] // 2
    pair_now = out_pair
    grad_now = out_grad
    pairs, grads, first_sums, second_sums, gain_sums = ([], [], [], [], [])
    for layer_index in range(N_SECTION - 1, -1, -1):
        results = coupling_back(pair_now[:, :channels], pair_now[:, channels:], grad_now[:, :channels].astype(jnp.float32), grad_now[:, channels:].astype(jnp.float32), f_weight[layer_index], g_weight[layer_index], gains[layer_index])
        pair_now = jnp.concatenate([results[0], results[1]], axis=1)
        grad_now = jnp.concatenate([results[2], results[3]], axis=1)
        pairs.append(pair_now)
        grads.append(grad_now)
        first_sums.append(replica_sum(results[4], results[5]))
        second_sums.append(replica_sum(results[6], results[7]))
        gain_sums.append(results[8])
    return (jnp.stack(pairs[::-1]), jnp.stack(grads[::-1]), jnp.stack(first_sums[::-1]), jnp.stack(second_sums[::-1]), jnp.stack(gain_sums[::-1]))
```

```python
import functools

import jax
import jax.numpy as jnp
from jax import lax
from jax.experimental import pallas as pl
from jax.experimental.pallas import tpu as pltpu
from jax.sharding import PartitionSpec as P

offset = 0.25
MESH = pl.DeviceIdType.MESH
f32, bf16 = jnp.float32, jnp.bfloat16


def silu_parts(pre_values):
    sigmoid_value = jax.nn.sigmoid(pre_values)
    return (pre_values * sigmoid_value, sigmoid_value * (1.0 + pre_values * (1.0 - sigmoid_value)))


def inverse_scale(values):
    return lax.rsqrt(jnp.mean(values * values, axis=-1, keepdims=True) + offset)


def kernel(
    n, sections, blocks,
    pair_ref, grad_ref, fw_ref, gw_ref, gains_ref,
    in_pair_ref, in_grad_ref, f_out, g_out, gain_out,
    wf, wg, rx, tx, held, slopes, norms_own, norms, deltas, gain_parts,
    own_sem, w_send, w_recv, p_send, p_recv, n_send, n_recv, d_send, d_recv, c_send, c_recv, out_sem,
):
    s, d = lax.axis_index("section"), lax.axis_index("dp")
    is_last = s == sections - 1
    has_below = s > 0
    not_last = jnp.logical_not(is_last)
    tokens = pair_ref.shape[0]
    h = pair_ref.shape[1] // 2
    part = fw_ref.shape[0]
    rows_per = tokens // blocks

    def peer(k):
        return lax.rem(d + k, n)

    barrier = pltpu.get_barrier_semaphore()
    for k in range(1, n):
        pl.semaphore_signal(barrier, inc=1, device_id=(s, peer(k)), device_id_type=MESH)

    @pl.when(has_below)
    def _():
        pl.semaphore_signal(barrier, inc=1, device_id=(s - 1, d), device_id_type=MESH)

    @pl.when(not_last)
    def _():
        pl.semaphore_signal(barrier, inc=1, device_id=(s + 1, d), device_id_type=MESH)

    neighbours = n - 1 + has_below.astype(jnp.int32) + not_last.astype(jnp.int32)
    pl.semaphore_wait(barrier, neighbours)

    fulls, owns = (wg, wf), (gw_ref, fw_ref)

    def shard(a, owner):
        return fulls[a].at[pl.ds(pl.multiple_of(owner * part, part), part)]

    def hop(a, way, k):
        owner = d - k if way == 0 else d + k
        src = owns[a] if k == 0 else shard(a, owner)
        return pltpu.make_async_remote_copy(
            src_ref=src, dst_ref=shard(a, owner),
            send_sem=w_send.at[a, way, k], recv_sem=w_recv.at[a, way, k],
            device_id=(s, d + 1 if way == 0 else d - 1), device_id_type=MESH,
        )

    def reach(way, k):
        if way == 0:
            return jnp.logical_and(d - k >= 0, d < n - 1)
        return jnp.logical_and(d + k < n, d > 0)

    def arrives(way, k):
        return d - k >= 0 if way == 0 else d + k < n

    for a in range(2):
        for way in range(2):
            @pl.when(reach(way, 0))
            def _():
                hop(a, way, 0).start()
    own_copies = [pltpu.make_async_copy(owns[a], shard(a, d), own_sem.at[a]) for a in range(2)]
    for copy in own_copies:
        copy.start()
    for k in range(1, n):
        for a in range(2):
            for way in range(2):
                @pl.when(arrives(way, k))
                def _():
                    owner = d - k if way == 0 else d + k
                    pltpu.make_async_remote_copy(
                        src_ref=owns[a], dst_ref=shard(a, owner),
                        send_sem=w_send.at[a, way, k - 1], recv_sem=w_recv.at[a, way, k - 1],
                        device_id=(s, d - 1 if way == 0 else d + 1), device_id_type=MESH,
                    ).wait_recv()

                if k < n - 1:
                    @pl.when(reach(way, k))
                    def _():
                        hop(a, way, k).start()
    for copy in own_copies:
        copy.wait()

    gain_out[...] = jnp.zeros_like(gain_out)

    def pair_copy(i, b):
        rows = pl.ds(pl.multiple_of(b * rows_per, rows_per), rows_per)
        return pltpu.make_async_remote_copy(
            src_ref=tx.at[i, rows], dst_ref=rx.at[i, rows],
            send_sem=p_send.at[i], recv_sem=p_recv.at[i, b],
            device_id=(s - 1, d), device_id_type=MESH,
        )

    def take(i, b, rows, source, column):
        @pl.when(is_last)
        def _():
            held[i] = source[rows, column].astype(f32)

        @pl.when(not_last)
        def _():
            rows_ = pl.ds(pl.multiple_of(b * rows_per, rows_per), rows_per)
            pltpu.make_async_remote_copy(
                src_ref=tx.at[i, rows_], dst_ref=rx.at[i, rows_],
                send_sem=p_send.at[i], recv_sem=p_recv.at[i, b],
                device_id=(s + 1, d), device_id_type=MESH,
            ).wait_recv()
            held[i] = rx[i, rows].astype(f32)

    def give(i, b, rows, values):
        tx[i, rows] = values.astype(bf16)

        @pl.when(has_below)
        def _():
            pair_copy(i, b).start()

    def share_norm(a, rows, normed):
        for e in range(n):
            norms_own[a, e, rows] = normed[:, e * part:(e + 1) * part]
        for k in range(1, n):
            e = peer(k)
            pltpu.make_async_remote_copy(
                src_ref=norms_own.at[a, e, rows], dst_ref=norms.at[a, d, rows],
                send_sem=n_send.at[a], recv_sem=n_recv.at[a],
                device_id=(s, e), device_id_type=MESH,
            ).start()

    def share_delta(a, rows, delta):
        deltas[a, d, rows] = delta
        for k in range(1, n):
            pltpu.make_async_remote_copy(
                src_ref=deltas.at[a, d, rows], dst_ref=deltas.at[a, d, rows],
                send_sem=d_send.at[a], recv_sem=d_recv.at[a],
                device_id=(s, peer(k)), device_id_type=MESH,
            ).start()

    first, second = pl.ds(0, h), pl.ds(h, h)
    trans = (((1,), (1,)), ((), ()))

    def block(b, carry):
        rows = pl.ds(pl.multiple_of(b * rows_per, rows_per), rows_per)
        gain_f, gain_g = gains_ref[0:1, :], gains_ref[1:2, :]
        take(0, b, rows, pair_ref, first)
        y1 = held[0]
        r1 = inverse_scale(y1)
        norm_g = (y1 * r1 * gain_g).astype(bf16)
        pre_g = jnp.dot(norm_g, wg[...], preferred_element_type=f32)
        take(1, b, rows, pair_ref, second)
        act_g, slope_g = silu_parts(pre_g)
        x2 = held[1] - act_g
        in_pair_ref[rows, second] = x2
        give(1, b, rows, x2)
        slopes[0] = slope_g
        r2 = inverse_scale(x2)
        norm_f = (x2 * r2 * gain_f).astype(bf16)
        pre_f = jnp.dot(norm_f, wf[...], preferred_element_type=f32)
        act_f, slope_f = silu_parts(pre_f)
        x1 = held[0] - act_f
        in_pair_ref[rows, first] = x1
        give(0, b, rows, x1)
        slopes[1] = slope_f
        share_norm(0, rows, norm_f)
        share_norm(1, rows, norm_g)

        take(3, b, rows, grad_ref, second)
        take(2, b, rows, grad_ref, first)
        delta_g = (held[3] * slopes[0]).astype(bf16)
        back_g = lax.dot_general(delta_g, wg[...], trans, preferred_element_type=f32)
        share_delta(1, rows, delta_g)
        y1 = held[0]
        weighted = gain_g * back_g
        gz = held[2] + r1 * weighted - y1 * (r1 * r1 * r1) * jnp.mean(
            weighted * y1, axis=-1, keepdims=True
        )
        in_grad_ref[rows, first] = gz.astype(bf16)
        give(2, b, rows, gz)
        gain_out[1:2, :] += jnp.sum(back_g * y1 * r1, axis=0, keepdims=True)
        delta_f = (gz * slopes[1]).astype(bf16)
        back_f = lax.dot_general(delta_f, wf[...], trans, preferred_element_type=f32)
        share_delta(0, rows, delta_f)
        x2 = in_pair_ref[rows, second]
        weighted = gain_f * back_f
        gx2 = held[3] + r2 * weighted - x2 * (r2 * r2 * r2) * jnp.mean(
            weighted * x2, axis=-1, keepdims=True
        )
        in_grad_ref[rows, second] = gx2.astype(bf16)
        give(3, b, rows, gx2)
        gain_out[0:1, :] += jnp.sum(back_f * x2 * r2, axis=0, keepdims=True)
        return carry

    lax.fori_loop(0, blocks, block, 0)

    gain_parts[d] = gain_out[...]
    for k in range(1, n):
        pltpu.make_async_remote_copy(
            src_ref=gain_parts.at[d], dst_ref=gain_parts.at[d],
            send_sem=c_send, recv_sem=c_recv,
            device_id=(s, peer(k)), device_id_type=MESH,
        ).start()

    def wait_bytes(ref, sem):
        pltpu.make_async_copy(ref, ref, sem).wait()

    for a in range(2):
        norms[a, d] = norms_own[a, d]
    others = pl.ds(0, n - 1)
    for a, out in ((1, g_out), (0, f_out)):
        wait_bytes(norms.at[a, others], n_recv.at[a])
        wait_bytes(deltas.at[a, others], d_recv.at[a])
        out[...] = lax.dot_general(
            norms[a].reshape(n * tokens, part), deltas[a].reshape(n * tokens, h),
            (((0,), (0,)), ((), ())), preferred_element_type=f32,
        )
    wait_bytes(gain_parts.at[others], c_recv)
    total = gain_parts[0]
    for e in range(1, n):
        total = total + gain_parts[e]
    gain_out[...] = total

    for a in range(2):
        wait_bytes(norms.at[a, others], n_send.at[a])
        wait_bytes(deltas.at[a, others], d_send.at[a])
    wait_bytes(gain_parts.at[others], c_send)

    @pl.when(has_below)
    def _():
        for i in range(4):
            wait_bytes(tx.at[i], p_send.at[i])

    for k in range(n - 1):
        for a in range(2):
            for way in range(2):
                @pl.when(reach(way, k))
                def _():
                    hop(a, way, k).wait_send()


def shards(out_pair, out_grad, f_weight, g_weight, gains):
    n, sections = lax.axis_size("dp"), lax.axis_size("section")
    tokens, width = out_pair.shape
    h = width // 2
    part = f_weight.shape[1]
    blocks = 4
    vmem = pl.BlockSpec(memory_space=pltpu.VMEM)
    dma = pltpu.SemaphoreType.DMA
    outs = pl.pallas_call(
        functools.partial(kernel, n, sections, blocks),
        out_shape=(
            jax.ShapeDtypeStruct((tokens, width), f32),
            jax.ShapeDtypeStruct((tokens, width), bf16),
            jax.ShapeDtypeStruct((part, h), f32),
            jax.ShapeDtypeStruct((part, h), f32),
            jax.ShapeDtypeStruct((2, h), f32),
        ),
        in_specs=[vmem] * 5,
        out_specs=[vmem] * 5,
        scratch_shapes=[
            pltpu.VMEM((h, h), bf16),
            pltpu.VMEM((h, h), bf16),
            pltpu.VMEM((4, tokens, h), bf16),
            pltpu.VMEM((4, tokens, h), bf16),
            pltpu.VMEM((4, tokens // blocks, h), f32),
            pltpu.VMEM((2, tokens // blocks, h), f32),
            pltpu.VMEM((2, n, tokens, part), bf16),
            pltpu.VMEM((2, n, tokens, part), bf16),
            pltpu.VMEM((2, n, tokens, h), bf16),
            pltpu.VMEM((n, 2, h), f32),
            dma((2,)),
            dma((2, 2, n)),
            dma((2, 2, n)),
            dma((4,)),
            dma((4, blocks)),
            dma((2,)),
            dma((2,)),
            dma((2,)),
            dma((2,)),
            dma,
            dma,
            dma,
        ],
        compiler_params=pltpu.CompilerParams(
            collective_id=0, has_side_effects=True, vmem_limit_bytes=60 * 1024 * 1024
        ),
    )(out_pair, out_grad, f_weight[0], g_weight[0], gains[0])
    return tuple(out[None] for out in outs)


def solution(mesh):
    placed = (
        P("dp", None),
        P("dp", None),
        P("section", "dp", None),
        P("section", "dp", None),
        P("section", None, None),
    )
    return jax.shard_map(
        shards,
        mesh=mesh,
        in_specs=placed,
        out_specs=(
            P("section", "dp", None),
            P("section", "dp", None),
            P("section", "dp", None),
            P("section", "dp", None),
            P("section", None, None),
        ),
        check_vma=False,
    )
```

```python
import functools

import jax
import jax.numpy as jnp
from jax import lax
from jax.experimental import pallas as pl
from jax.experimental.pallas import tpu as pltpu
from jax.sharding import PartitionSpec as P

offset = 0.25
MESH = pl.DeviceIdType.MESH
f32, bf16 = jnp.float32, jnp.bfloat16


def silu_parts(pre_values):
    sigmoid_value = jax.nn.sigmoid(pre_values)
    return (pre_values * sigmoid_value, sigmoid_value * (1.0 + pre_values * (1.0 - sigmoid_value)))


def inverse_scale(values):
    return lax.rsqrt(jnp.mean(values * values, axis=-1, keepdims=True) + offset)


def kernel(
    n, sections, blocks,
    pair_ref, grad_ref, fw_ref, gw_ref, gains_ref,
    in_pair_ref, in_grad_ref, f_out, g_out, gain_out,
    wf, wg, rx, tx, held, slopes, norms_own, norms, deltas, gain_parts,
    own_sem, w_send, w_recv, p_send, p_recv, n_send, n_recv, d_send, d_recv, c_send, c_recv,
):
    s, d = lax.axis_index("section"), lax.axis_index("dp")
    is_last = s == sections - 1
    has_below = s > 0
    not_last = jnp.logical_not(is_last)
    tokens = pair_ref.shape[0]
    h = pair_ref.shape[1] // 2
    part = fw_ref.shape[0]
    rows_per = tokens // blocks

    def peer(k):
        return lax.rem(d + k, n)

    barrier = pltpu.get_barrier_semaphore()
    for k in range(1, n):
        pl.semaphore_signal(barrier, inc=1, device_id=(s, peer(k)), device_id_type=MESH)

    @pl.when(has_below)
    def _():
        pl.semaphore_signal(barrier, inc=1, device_id=(s - 1, d), device_id_type=MESH)

    @pl.when(not_last)
    def _():
        pl.semaphore_signal(barrier, inc=1, device_id=(s + 1, d), device_id_type=MESH)

    neighbours = n - 1 + has_below.astype(jnp.int32) + not_last.astype(jnp.int32)
    pl.semaphore_wait(barrier, neighbours)

    fulls, owns = (wg, wf), (gw_ref, fw_ref)

    def shard(a, owner):
        return fulls[a].at[pl.ds(pl.multiple_of(owner * part, part), part)]

    def hop(a, way, k):
        owner = d - k if way == 0 else d + k
        src = owns[a] if k == 0 else shard(a, owner)
        return pltpu.make_async_remote_copy(
            src_ref=src, dst_ref=shard(a, owner),
            send_sem=w_send.at[a, way, k], recv_sem=w_recv.at[a, way, k],
            device_id=(s, d + 1 if way == 0 else d - 1), device_id_type=MESH,
        )

    def reach(way, k):
        if way == 0:
            return jnp.logical_and(d - k >= 0, d < n - 1)
        return jnp.logical_and(d + k < n, d > 0)

    def arrives(way, k):
        return d - k >= 0 if way == 0 else d + k < n

    for a in range(2):
        for way in range(2):
            @pl.when(reach(way, 0))
            def _():
                hop(a, way, 0).start()
    own_copies = [pltpu.make_async_copy(owns[a], shard(a, d), own_sem.at[a]) for a in range(2)]
    for copy in own_copies:
        copy.start()
    for k in range(1, n):
        for a in range(2):
            for way in range(2):
                @pl.when(arrives(way, k))
                def _():
                    owner = d - k if way == 0 else d + k
                    pltpu.make_async_remote_copy(
                        src_ref=owns[a], dst_ref=shard(a, owner),
                        send_sem=w_send.at[a, way, k - 1], recv_sem=w_recv.at[a, way, k - 1],
                        device_id=(s, d - 1 if way == 0 else d + 1), device_id_type=MESH,
                    ).wait_recv()

                if k < n - 1:
                    @pl.when(reach(way, k))
                    def _():
                        hop(a, way, k).start()
    for copy in own_copies:
        copy.wait()

    gain_out[...] = jnp.zeros_like(gain_out)

    def pair_copy(i, b):
        rows = pl.ds(pl.multiple_of(b * rows_per, rows_per), rows_per)
        return pltpu.make_async_remote_copy(
            src_ref=tx.at[i, rows], dst_ref=rx.at[i, rows],
            send_sem=p_send.at[i], recv_sem=p_recv.at[i, b],
            device_id=(s - 1, d), device_id_type=MESH,
        )

    def take(i, b, rows, source, column):
        @pl.when(is_last)
        def _():
            held[i] = source[rows, column].astype(f32)

        @pl.when(not_last)
        def _():
            rows_ = pl.ds(pl.multiple_of(b * rows_per, rows_per), rows_per)
            pltpu.make_async_remote_copy(
                src_ref=tx.at[i, rows_], dst_ref=rx.at[i, rows_],
                send_sem=p_send.at[i], recv_sem=p_recv.at[i, b],
                device_id=(s + 1, d), device_id_type=MESH,
            ).wait_recv()
            held[i] = rx[i, rows].astype(f32)

    def give(i, b, rows, values):
        tx[i, rows] = values.astype(bf16)

        @pl.when(has_below)
        def _():
            pair_copy(i, b).start()

    def share_norm(a, rows, normed):
        for e in range(n):
            norms_own[a, e, rows] = normed[:, e * part:(e + 1) * part]
        for k in range(1, n):
            e = peer(k)
            pltpu.make_async_remote_copy(
                src_ref=norms_own.at[a, e, rows], dst_ref=norms.at[a, d, rows],
                send_sem=n_send.at[a], recv_sem=n_recv.at[a],
                device_id=(s, e), device_id_type=MESH,
            ).start()

    def delta_hop(a, way, k, rows):
        owner = d - k if way == 0 else d + k
        return pltpu.make_async_remote_copy(
            src_ref=deltas.at[a, owner, rows], dst_ref=deltas.at[a, owner, rows],
            send_sem=d_send.at[a, way, k], recv_sem=d_recv.at[a, way, k],
            device_id=(s, d + 1 if way == 0 else d - 1), device_id_type=MESH,
        )

    def share_delta(a, rows, delta):
        deltas[a, d, rows] = delta
        for way in range(2):
            @pl.when(reach(way, 0))
            def _():
                delta_hop(a, way, 0, rows).start()

    first, second = pl.ds(0, h), pl.ds(h, h)
    trans = (((1,), (1,)), ((), ()))

    def block(b, carry):
        rows = pl.ds(pl.multiple_of(b * rows_per, rows_per), rows_per)
        gain_f, gain_g = gains_ref[0:1, :], gains_ref[1:2, :]
        take(0, b, rows, pair_ref, first)
        y1 = held[0]
        r1 = inverse_scale(y1)
        norm_g = (y1 * r1 * gain_g).astype(bf16)
        pre_g = jnp.dot(norm_g, wg[...], preferred_element_type=f32)
        take(1, b, rows, pair_ref, second)
        act_g, slope_g = silu_parts(pre_g)
        x2 = held[1] - act_g
        in_pair_ref[rows, second] = x2
        give(1, b, rows, x2)
        slopes[0] = slope_g
        r2 = inverse_scale(x2)
        norm_f = (x2 * r2 * gain_f).astype(bf16)
        pre_f = jnp.dot(norm_f, wf[...], preferred_element_type=f32)
        act_f, slope_f = silu_parts(pre_f)
        x1 = held[0] - act_f
        in_pair_ref[rows, first] = x1
        give(0, b, rows, x1)
        slopes[1] = slope_f
        share_norm(0, rows, norm_f)
        share_norm(1, rows, norm_g)

        take(3, b, rows, grad_ref, second)
        take(2, b, rows, grad_ref, first)
        delta_g = (held[3] * slopes[0]).astype(bf16)
        back_g = lax.dot_general(delta_g, wg[...], trans, preferred_element_type=f32)
        share_delta(1, rows, delta_g)
        y1 = held[0]
        weighted = gain_g * back_g
        gz = held[2] + r1 * weighted - y1 * (r1 * r1 * r1) * jnp.mean(
            weighted * y1, axis=-1, keepdims=True
        )
        in_grad_ref[rows, first] = gz.astype(bf16)
        give(2, b, rows, gz)
        gain_out[1:2, :] += jnp.sum(back_g * y1 * r1, axis=0, keepdims=True)
        delta_f = (gz * slopes[1]).astype(bf16)
        back_f = lax.dot_general(delta_f, wf[...], trans, preferred_element_type=f32)
        share_delta(0, rows, delta_f)
        x2 = in_pair_ref[rows, second]
        weighted = gain_f * back_f
        gx2 = held[3] + r2 * weighted - x2 * (r2 * r2 * r2) * jnp.mean(
            weighted * x2, axis=-1, keepdims=True
        )
        in_grad_ref[rows, second] = gx2.astype(bf16)
        give(3, b, rows, gx2)
        gain_out[0:1, :] += jnp.sum(back_f * x2 * r2, axis=0, keepdims=True)
        return carry

    lax.fori_loop(0, blocks, block, 0)

    gain_parts[d] = gain_out[...]
    for k in range(1, n):
        pltpu.make_async_remote_copy(
            src_ref=gain_parts.at[d], dst_ref=gain_parts.at[d],
            send_sem=c_send, recv_sem=c_recv,
            device_id=(s, peer(k)), device_id_type=MESH,
        ).start()

    def wait_bytes(ref, sem):
        pltpu.make_async_copy(ref, ref, sem).wait()

    for a in range(2):
        norms[a, d] = norms_own[a, d]
    others, whole = pl.ds(0, n - 1), pl.ds(0, tokens)
    for k in range(1, n):
        for a, out in ((1, g_out), (0, f_out)):
            for way in range(2):
                @pl.when(arrives(way, k))
                def _():
                    wait_bytes(deltas.at[a, d - k if way == 0 else d + k], d_recv.at[a, way, k - 1])

                if k < n - 1:
                    @pl.when(reach(way, k))
                    def _():
                        delta_hop(a, way, k, whole).start()
            if k == n - 1:
                wait_bytes(norms.at[a, others], n_recv.at[a])
                out[...] = lax.dot_general(
                    norms[a].reshape(n * tokens, part), deltas[a].reshape(n * tokens, h),
                    (((0,), (0,)), ((), ())), preferred_element_type=f32,
                )
    wait_bytes(gain_parts.at[others], c_recv)
    total = gain_parts[0]
    for e in range(1, n):
        total = total + gain_parts[e]
    gain_out[...] = total

    for a in range(2):
        wait_bytes(norms.at[a, others], n_send.at[a])
        for k in range(n - 1):
            for way in range(2):
                @pl.when(reach(way, k))
                def _():
                    wait_bytes(deltas.at[a, d - k if way == 0 else d + k], d_send.at[a, way, k])
    wait_bytes(gain_parts.at[others], c_send)

    @pl.when(has_below)
    def _():
        for i in range(4):
            wait_bytes(tx.at[i], p_send.at[i])

    for k in range(n - 1):
        for a in range(2):
            for way in range(2):
                @pl.when(reach(way, k))
                def _():
                    hop(a, way, k).wait_send()


def shards(out_pair, out_grad, f_weight, g_weight, gains):
    n, sections = lax.axis_size("dp"), lax.axis_size("section")
    tokens, width = out_pair.shape
    h = width // 2
    part = f_weight.shape[1]
    blocks = 4
    vmem = pl.BlockSpec(memory_space=pltpu.VMEM)
    dma = pltpu.SemaphoreType.DMA
    outs = pl.pallas_call(
        functools.partial(kernel, n, sections, blocks),
        out_shape=(
            jax.ShapeDtypeStruct((tokens, width), f32),
            jax.ShapeDtypeStruct((tokens, width), bf16),
            jax.ShapeDtypeStruct((part, h), f32),
            jax.ShapeDtypeStruct((part, h), f32),
            jax.ShapeDtypeStruct((2, h), f32),
        ),
        in_specs=[vmem] * 5,
        out_specs=[vmem] * 5,
        scratch_shapes=[
            pltpu.VMEM((h, h), bf16),
            pltpu.VMEM((h, h), bf16),
            pltpu.VMEM((4, tokens, h), bf16),
            pltpu.VMEM((4, tokens, h), bf16),
            pltpu.VMEM((4, tokens // blocks, h), f32),
            pltpu.VMEM((2, tokens // blocks, h), f32),
            pltpu.VMEM((2, n, tokens, part), bf16),
            pltpu.VMEM((2, n, tokens, part), bf16),
            pltpu.VMEM((2, n, tokens, h), bf16),
            pltpu.VMEM((n, 2, h), f32),
            dma((2,)),
            dma((2, 2, n)),
            dma((2, 2, n)),
            dma((4,)),
            dma((4, blocks)),
            dma((2,)),
            dma((2,)),
            dma((2, 2, n)),
            dma((2, 2, n)),
            dma,
            dma,
        ],
        compiler_params=pltpu.CompilerParams(
            collective_id=0, has_side_effects=True, vmem_limit_bytes=60 * 1024 * 1024
        ),
    )(out_pair, out_grad, f_weight[0], g_weight[0], gains[0])
    return tuple(out[None] for out in outs)


def solution(mesh):
    placed = (
        P("dp", None),
        P("dp", None),
        P("section", "dp", None),
        P("section", "dp", None),
        P("section", None, None),
    )
    return jax.shard_map(
        shards,
        mesh=mesh,
        in_specs=placed,
        out_specs=(
            P("section", "dp", None),
            P("section", "dp", None),
            P("section", "dp", None),
            P("section", "dp", None),
            P("section", None, None),
        ),
        check_vma=False,
    )
```

```python
import functools

import jax
import jax.numpy as jnp
from jax import lax
from jax.experimental import pallas as pl
from jax.experimental.pallas import tpu as pltpu
from jax.sharding import PartitionSpec as P

offset = 0.25
MESH = pl.DeviceIdType.MESH
f32, bf16 = jnp.float32, jnp.bfloat16


def silu_parts(pre_values):
    sigmoid_value = jax.nn.sigmoid(pre_values)
    return (pre_values * sigmoid_value, sigmoid_value * (1.0 + pre_values * (1.0 - sigmoid_value)))


def inverse_scale(values):
    return lax.rsqrt(jnp.mean(values * values, axis=-1, keepdims=True) + offset)


def kernel(
    n, sections, blocks,
    pair_ref, grad_ref, fw_ref, gw_ref, gains_ref,
    in_pair_ref, in_grad_ref, f_out, g_out, gain_out,
    wf, wg, wft, wgt, aside, rx, tx, held, slopes, norms_own, norms, deltas, gain_parts,
    own_sem, i_send, i_recv, h_send, h_recv, o_send, o_recv, w_send, w_recv, p_send, p_recv, n_send, n_recv, d_send, d_recv, c_send, c_recv,
):
    s, d = lax.axis_index("section"), lax.axis_index("dp")
    is_last = s == sections - 1
    has_below = s > 0
    not_last = jnp.logical_not(is_last)
    tokens = pair_ref.shape[0]
    h = pair_ref.shape[1] // 2
    part = fw_ref.shape[0]
    rows_per = tokens // blocks

    def peer(k):
        return lax.rem(d + k, n)

    barrier = pltpu.get_barrier_semaphore()
    for k in range(1, n):
        pl.semaphore_signal(barrier, inc=1, device_id=(s, peer(k)), device_id_type=MESH)

    @pl.when(has_below)
    def _():
        pl.semaphore_signal(barrier, inc=1, device_id=(s - 1, d), device_id_type=MESH)

    @pl.when(not_last)
    def _():
        pl.semaphore_signal(barrier, inc=1, device_id=(s + 1, d), device_id_type=MESH)

    half = sections // 2
    partner = lax.rem(s + half, sections)
    high, low = s >= half, s < half
    pl.semaphore_signal(barrier, inc=1, device_id=(partner, d), device_id_type=MESH)
    neighbours = n + has_below.astype(jnp.int32) + not_last.astype(jnp.int32)
    pl.semaphore_wait(barrier, neighbours)

    fulls, owns, turned = (wg, wf), (gw_ref, fw_ref), (wgt, wft)
    keep = h - aside.shape[3]
    variants = ((low, pl.ds(0, h)), (high, pl.ds(0, keep)))
    rest = pl.ds(keep, h - keep)

    def shard(a, owner, cols):
        return fulls[a].at[pl.ds(pl.multiple_of(owner * part, part), part), cols]

    def owner_of(way, k):
        return d - k if way == 0 else d + k

    def ahead(way):
        return d + 1 if way == 0 else d - 1

    def hop(a, way, k, cols):
        owner = owner_of(way, k)
        src = owns[a].at[:, cols] if k == 0 else shard(a, owner, cols)
        return pltpu.make_async_remote_copy(
            src_ref=src, dst_ref=shard(a, owner, cols),
            send_sem=w_send.at[a, way, k], recv_sem=w_recv.at[a, way, k],
            device_id=(s, ahead(way)), device_id_type=MESH,
        )

    def aside_in(a):
        return pltpu.make_async_remote_copy(
            src_ref=owns[a].at[:, rest], dst_ref=aside.at[a, d],
            send_sem=i_send.at[a], recv_sem=i_recv.at[a],
            device_id=(partner, d), device_id_type=MESH,
        )

    def aside_hop(a, way, k):
        owner = owner_of(way, k)
        return pltpu.make_async_remote_copy(
            src_ref=aside.at[a, owner], dst_ref=aside.at[a, owner],
            send_sem=h_send.at[a, way, k], recv_sem=h_recv.at[a, way, k],
            device_id=(s, ahead(way)), device_id_type=MESH,
        )

    def aside_out(a, way, k):
        owner = owner_of(way, k)
        return pltpu.make_async_remote_copy(
            src_ref=aside.at[a, owner], dst_ref=shard(a, owner, rest),
            send_sem=o_send.at[a, way, k], recv_sem=o_recv.at[a, way, k],
            device_id=(partner, d), device_id_type=MESH,
        )

    def wait_bytes(ref, sem):
        pltpu.make_async_copy(ref, ref, sem).wait()

    def reach(way, k):
        if way == 0:
            return jnp.logical_and(d - k >= 0, d < n - 1)
        return jnp.logical_and(d + k < n, d > 0)

    def arrives(way, k):
        return d - k >= 0 if way == 0 else d + k < n

    both = jnp.logical_and

    @pl.when(high)
    def _():
        for a in range(2):
            aside_in(a).start()

    @pl.when(low)
    def _():
        for a in range(2):
            wait_bytes(aside.at[a, d], i_recv.at[a])
            for way in range(2):
                @pl.when(reach(way, 0))
                def _():
                    aside_hop(a, way, 0).start()

    for a in range(2):
        for way in range(2):
            for side, cols in variants:
                @pl.when(both(side, reach(way, 0)))
                def _():
                    hop(a, way, 0, cols).start()
    early = part % 128 == 0

    def turn(a, owner):
        span = pl.ds(pl.multiple_of(owner * part, part), part)
        turned[a][:, span] = fulls[a][span, :].T

    own_copies = [
        pltpu.make_async_copy(owns[a], shard(a, d, pl.ds(0, h)), own_sem.at[a]) for a in range(2)
    ]
    for copy in own_copies:
        copy.start()
    for a, copy in enumerate(own_copies):
        copy.wait()
        if early:
            turn(a, d)
    for k in range(1, n):
        for a in range(2):
            for way in range(2):
                @pl.when(both(low, arrives(way, k)))
                def _():
                    wait_bytes(aside.at[a, owner_of(way, k)], h_recv.at[a, way, k - 1])
                    if k < n - 1:
                        @pl.when(reach(way, k))
                        def _():
                            aside_hop(a, way, k).start()
                    aside_out(a, way, k).start()
        for a in range(2):
            for way in range(2):
                for side, cols in variants:
                    @pl.when(both(side, arrives(way, k)))
                    def _():
                        wait_bytes(shard(a, owner_of(way, k), cols), w_recv.at[a, way, k - 1])

                    if k < n - 1:
                        @pl.when(both(side, reach(way, k)))
                        def _():
                            hop(a, way, k, cols).start()
        for a in range(2):
            for way in range(2):
                @pl.when(both(high, arrives(way, k)))
                def _():
                    wait_bytes(shard(a, owner_of(way, k), rest), o_recv.at[a, way, k])

                if early:
                    @pl.when(arrives(way, k))
                    def _():
                        turn(a, owner_of(way, k))
    if not early:
        for a in range(2):
            turned[a][...] = fulls[a][...].T

    gain_out[...] = jnp.zeros_like(gain_out)

    def pair_copy(i, b):
        rows = pl.ds(pl.multiple_of(b * rows_per, rows_per), rows_per)
        return pltpu.make_async_remote_copy(
            src_ref=tx.at[i, rows], dst_ref=rx.at[i, rows],
            send_sem=p_send.at[i], recv_sem=p_recv.at[i, b],
            device_id=(s - 1, d), device_id_type=MESH,
        )

    def take(i, b, rows, source, column):
        @pl.when(is_last)
        def _():
            held[i] = source[rows, column].astype(f32)

        @pl.when(not_last)
        def _():
            rows_ = pl.ds(pl.multiple_of(b * rows_per, rows_per), rows_per)
            pltpu.make_async_remote_copy(
                src_ref=tx.at[i, rows_], dst_ref=rx.at[i, rows_],
                send_sem=p_send.at[i], recv_sem=p_recv.at[i, b],
                device_id=(s + 1, d), device_id_type=MESH,
            ).wait_recv()
            held[i] = rx[i, rows].astype(f32)

    def give(i, b, rows, values):
        tx[i, rows] = values.astype(bf16)

        @pl.when(has_below)
        def _():
            pair_copy(i, b).start()

    def share_norm(a, rows, normed):
        for e in range(n):
            norms_own[a, e, rows] = normed[:, e * part:(e + 1) * part]
        for k in range(1, n):
            e = peer(k)
            pltpu.make_async_remote_copy(
                src_ref=norms_own.at[a, e, rows], dst_ref=norms.at[a, d, rows],
                send_sem=n_send.at[a], recv_sem=n_recv.at[a],
                device_id=(s, e), device_id_type=MESH,
            ).start()

    def delta_hop(a, way, k, rows):
        owner = d - k if way == 0 else d + k
        return pltpu.make_async_remote_copy(
            src_ref=deltas.at[a, owner, rows], dst_ref=deltas.at[a, owner, rows],
            send_sem=d_send.at[a, way, k], recv_sem=d_recv.at[a, way, k],
            device_id=(s, d + 1 if way == 0 else d - 1), device_id_type=MESH,
        )

    def share_delta(a, rows, delta):
        deltas[a, d, rows] = delta
        for way in range(2):
            @pl.when(reach(way, 0))
            def _():
                delta_hop(a, way, 0, rows).start()

    first, second = pl.ds(0, h), pl.ds(h, h)

    def block(b, carry):
        rows = pl.ds(pl.multiple_of(b * rows_per, rows_per), rows_per)
        gain_f, gain_g = gains_ref[0:1, :], gains_ref[1:2, :]
        take(0, b, rows, pair_ref, first)
        y1 = held[0]
        r1 = inverse_scale(y1)
        norm_g = (y1 * r1 * gain_g).astype(bf16)
        pre_g = jnp.dot(norm_g, wg[...], preferred_element_type=f32)
        take(1, b, rows, pair_ref, second)
        act_g, slope_g = silu_parts(pre_g)
        x2 = held[1] - act_g
        in_pair_ref[rows, second] = x2
        give(1, b, rows, x2)
        slopes[0] = slope_g
        r2 = inverse_scale(x2)
        norm_f = (x2 * r2 * gain_f).astype(bf16)
        pre_f = jnp.dot(norm_f, wf[...], preferred_element_type=f32)
        act_f, slope_f = silu_parts(pre_f)
        x1 = held[0] - act_f
        in_pair_ref[rows, first] = x1
        give(0, b, rows, x1)
        slopes[1] = slope_f
        share_norm(0, rows, norm_f)
        share_norm(1, rows, norm_g)

        take(3, b, rows, grad_ref, second)
        take(2, b, rows, grad_ref, first)
        delta_g = (held[3] * slopes[0]).astype(bf16)
        back_g = jnp.dot(delta_g, wgt[...], preferred_element_type=f32)
        share_delta(1, rows, delta_g)
        y1 = held[0]
        weighted = gain_g * back_g
        gz = held[2] + r1 * weighted - y1 * (r1 * r1 * r1) * jnp.mean(
            weighted * y1, axis=-1, keepdims=True
        )
        in_grad_ref[rows, first] = gz.astype(bf16)
        give(2, b, rows, gz)
        gain_out[1:2, :] += jnp.sum(back_g * y1 * r1, axis=0, keepdims=True)
        delta_f = (gz * slopes[1]).astype(bf16)
        back_f = jnp.dot(delta_f, wft[...], preferred_element_type=f32)
        share_delta(0, rows, delta_f)
        x2 = in_pair_ref[rows, second]
        weighted = gain_f * back_f
        gx2 = held[3] + r2 * weighted - x2 * (r2 * r2 * r2) * jnp.mean(
            weighted * x2, axis=-1, keepdims=True
        )
        in_grad_ref[rows, second] = gx2.astype(bf16)
        give(3, b, rows, gx2)
        gain_out[0:1, :] += jnp.sum(back_f * x2 * r2, axis=0, keepdims=True)
        return carry

    lax.fori_loop(0, blocks, block, 0)

    gain_parts[d] = gain_out[...]
    for k in range(1, n):
        pltpu.make_async_remote_copy(
            src_ref=gain_parts.at[d], dst_ref=gain_parts.at[d],
            send_sem=c_send, recv_sem=c_recv,
            device_id=(s, peer(k)), device_id_type=MESH,
        ).start()

    for a in range(2):
        norms[a, d] = norms_own[a, d]
    others, whole = pl.ds(0, n - 1), pl.ds(0, tokens)
    for k in range(1, n):
        for a, out in ((1, g_out), (0, f_out)):
            for way in range(2):
                @pl.when(arrives(way, k))
                def _():
                    wait_bytes(deltas.at[a, d - k if way == 0 else d + k], d_recv.at[a, way, k - 1])

                if k < n - 1:
                    @pl.when(reach(way, k))
                    def _():
                        delta_hop(a, way, k, whole).start()
            if k == n - 1:
                wait_bytes(norms.at[a, others], n_recv.at[a])
                out[...] = lax.dot_general(
                    norms[a].reshape(n * tokens, part), deltas[a].reshape(n * tokens, h),
                    (((0,), (0,)), ((), ())), preferred_element_type=f32,
                )
    wait_bytes(gain_parts.at[others], c_recv)
    total = gain_parts[0]
    for e in range(1, n):
        total = total + gain_parts[e]
    gain_out[...] = total

    for a in range(2):
        wait_bytes(norms.at[a, others], n_send.at[a])
        for k in range(n - 1):
            for way in range(2):
                @pl.when(reach(way, k))
                def _():
                    wait_bytes(deltas.at[a, d - k if way == 0 else d + k], d_send.at[a, way, k])
    wait_bytes(gain_parts.at[others], c_send)

    @pl.when(has_below)
    def _():
        for i in range(4):
            wait_bytes(tx.at[i], p_send.at[i])

    @pl.when(high)
    def _():
        for a in range(2):
            aside_in(a).wait_send()

    for k in range(n):
        for a in range(2):
            for way in range(2):
                if k < n - 1:
                    for side, cols in variants:
                        @pl.when(both(side, reach(way, k)))
                        def _():
                            hop(a, way, k, cols).wait_send()

                    @pl.when(both(low, reach(way, k)))
                    def _():
                        aside_hop(a, way, k).wait_send()
                if k > 0:
                    @pl.when(both(low, arrives(way, k)))
                    def _():
                        aside_out(a, way, k).wait_send()


def shards(out_pair, out_grad, f_weight, g_weight, gains):
    n, sections = lax.axis_size("dp"), lax.axis_size("section")
    tokens, width = out_pair.shape
    h = width // 2
    part = f_weight.shape[1]
    blocks = 4
    vmem = pl.BlockSpec(memory_space=pltpu.VMEM)
    dma = pltpu.SemaphoreType.DMA
    outs = pl.pallas_call(
        functools.partial(kernel, n, sections, blocks),
        out_shape=(
            jax.ShapeDtypeStruct((tokens, width), f32),
            jax.ShapeDtypeStruct((tokens, width), bf16),
            jax.ShapeDtypeStruct((part, h), f32),
            jax.ShapeDtypeStruct((part, h), f32),
            jax.ShapeDtypeStruct((2, h), f32),
        ),
        in_specs=[vmem] * 5,
        out_specs=[vmem] * 5,
        scratch_shapes=[
            pltpu.VMEM((h, h), bf16),
            pltpu.VMEM((h, h), bf16),
            pltpu.VMEM((h, h), bf16),
            pltpu.VMEM((h, h), bf16),
            pltpu.VMEM((2, n, part, h // 8), bf16),
            pltpu.VMEM((4, tokens, h), bf16),
            pltpu.VMEM((4, tokens, h), bf16),
            pltpu.VMEM((4, tokens // blocks, h), f32),
            pltpu.VMEM((2, tokens // blocks, h), f32),
            pltpu.VMEM((2, n, tokens, part), bf16),
            pltpu.VMEM((2, n, tokens, part), bf16),
            pltpu.VMEM((2, n, tokens, h), bf16),
            pltpu.VMEM((n, 2, h), f32),
            dma((2,)),
            dma((2,)),
            dma((2,)),
            dma((2, 2, n)),
            dma((2, 2, n)),
            dma((2, 2, n)),
            dma((2, 2, n)),
            dma((2, 2, n)),
            dma((2, 2, n)),
            dma((4,)),
            dma((4, blocks)),
            dma((2,)),
            dma((2,)),
            dma((2, 2, n)),
            dma((2, 2, n)),
            dma,
            dma,
        ],
        compiler_params=pltpu.CompilerParams(
            collective_id=0, has_side_effects=True, vmem_limit_bytes=60 * 1024 * 1024
        ),
    )(out_pair, out_grad, f_weight[0], g_weight[0], gains[0])
    return tuple(out[None] for out in outs)


def solution(mesh):
    placed = (
        P("dp", None),
        P("dp", None),
        P("section", "dp", None),
        P("section", "dp", None),
        P("section", None, None),
    )
    return jax.shard_map(
        shards,
        mesh=mesh,
        in_specs=placed,
        out_specs=(
            P("section", "dp", None),
            P("section", "dp", None),
            P("section", "dp", None),
            P("section", "dp", None),
            P("section", None, None),
        ),
        check_vma=False,
    )
```

```python
import functools

import jax
import jax.numpy as jnp
from jax import lax
from jax.experimental import pallas as pl
from jax.experimental.pallas import tpu as pltpu
from jax.sharding import PartitionSpec as P

offset = 0.25
MESH = pl.DeviceIdType.MESH
f32, bf16 = jnp.float32, jnp.bfloat16


def silu_parts(pre_values):
    sigmoid_value = jax.nn.sigmoid(pre_values)
    return (pre_values * sigmoid_value, sigmoid_value * (1.0 + pre_values * (1.0 - sigmoid_value)))


def inverse_scale(values):
    return lax.rsqrt(jnp.mean(values * values, axis=-1, keepdims=True) + offset)


def kernel(
    n, sections, blocks,
    pair_ref, grad_ref, fw_ref, gw_ref, gains_ref,
    in_pair_ref, in_grad_ref, f_out, g_out, gain_out,
    wf, wg, wft, wgt, aside, late, rx, tx, held, slopes, norms_own, norms, deltas, gain_parts,
    l_sem, lh_send, lh_recv, lo_send, lo_recv, own_sem, i_send, i_recv, h_send, h_recv, o_send, o_recv, w_send, w_recv, p_send, p_recv, n_send, n_recv, d_send, d_recv, c_send, c_recv,
):
    s, d = lax.axis_index("section"), lax.axis_index("dp")
    is_last = s == sections - 1
    has_below = s > 0
    not_last = jnp.logical_not(is_last)
    tokens = pair_ref.shape[0]
    h = pair_ref.shape[1] // 2
    part = fw_ref.shape[0]
    rows_per = tokens // blocks

    def peer(k):
        return lax.rem(d + k, n)

    barrier = pltpu.get_barrier_semaphore()
    for k in range(1, n):
        pl.semaphore_signal(barrier, inc=1, device_id=(s, peer(k)), device_id_type=MESH)

    @pl.when(has_below)
    def _():
        pl.semaphore_signal(barrier, inc=1, device_id=(s - 1, d), device_id_type=MESH)

    @pl.when(not_last)
    def _():
        pl.semaphore_signal(barrier, inc=1, device_id=(s + 1, d), device_id_type=MESH)

    half = sections // 2
    partner = lax.rem(s + half, sections)
    high, low = s >= half, s < half
    pl.semaphore_signal(barrier, inc=1, device_id=(partner, d), device_id_type=MESH)
    neighbours = n + has_below.astype(jnp.int32) + not_last.astype(jnp.int32)
    pl.semaphore_wait(barrier, neighbours)

    fulls, owns, turned = (wg, wf), (gw_ref, fw_ref), (wgt, wft)
    keep = h - aside.shape[3]
    variants = ((low, pl.ds(0, h)), (high, pl.ds(0, keep)))
    rest = pl.ds(keep, h - keep)

    def shard(a, owner, cols):
        return fulls[a].at[pl.ds(pl.multiple_of(owner * part, part), part), cols]

    def owner_of(way, k):
        return d - k if way == 0 else d + k

    def ahead(way):
        return d + 1 if way == 0 else d - 1

    def hop(a, way, k, cols):
        owner = owner_of(way, k)
        src = owns[a].at[:, cols] if k == 0 else shard(a, owner, cols)
        return pltpu.make_async_remote_copy(
            src_ref=src, dst_ref=shard(a, owner, cols),
            send_sem=w_send.at[a, way, k], recv_sem=w_recv.at[a, way, k],
            device_id=(s, ahead(way)), device_id_type=MESH,
        )

    def aside_in(a):
        return pltpu.make_async_remote_copy(
            src_ref=owns[a].at[:, rest], dst_ref=aside.at[a, d],
            send_sem=i_send.at[a], recv_sem=i_recv.at[a],
            device_id=(partner, d), device_id_type=MESH,
        )

    def aside_hop(a, way, k):
        owner = owner_of(way, k)
        return pltpu.make_async_remote_copy(
            src_ref=aside.at[a, owner], dst_ref=aside.at[a, owner],
            send_sem=h_send.at[a, way, k], recv_sem=h_recv.at[a, way, k],
            device_id=(s, ahead(way)), device_id_type=MESH,
        )

    def aside_out(a, way, k):
        owner = owner_of(way, k)
        return pltpu.make_async_remote_copy(
            src_ref=aside.at[a, owner], dst_ref=shard(a, owner, rest),
            send_sem=o_send.at[a, way, k], recv_sem=o_recv.at[a, way, k],
            device_id=(partner, d), device_id_type=MESH,
        )

    def wait_bytes(ref, sem):
        pltpu.make_async_copy(ref, ref, sem).wait()

    def reach(way, k):
        if way == 0:
            return jnp.logical_and(d - k >= 0, d < n - 1)
        return jnp.logical_and(d + k < n, d > 0)

    def arrives(way, k):
        return d - k >= 0 if way == 0 else d + k < n

    both = jnp.logical_and

    @pl.when(high)
    def _():
        for a in range(2):
            aside_in(a).start()

    @pl.when(low)
    def _():
        for a in range(2):
            wait_bytes(aside.at[a, d], i_recv.at[a])
            for way in range(2):
                @pl.when(reach(way, 0))
                def _():
                    aside_hop(a, way, 0).start()

    for a in range(2):
        for way in range(2):
            for side, cols in variants:
                @pl.when(both(side, reach(way, 0)))
                def _():
                    hop(a, way, 0, cols).start()
    early = part % 128 == 0

    def turn(a, owner):
        span = pl.ds(pl.multiple_of(owner * part, part), part)
        turned[a][:, span] = fulls[a][span, :].T

    own_copies = [
        pltpu.make_async_copy(owns[a], shard(a, d, pl.ds(0, h)), own_sem.at[a]) for a in range(2)
    ]
    for copy in own_copies:
        copy.start()
    for a, copy in enumerate(own_copies):
        copy.wait()
        if early:
            turn(a, d)
    for k in range(1, n):
        for a in range(2):
            for way in range(2):
                @pl.when(both(low, arrives(way, k)))
                def _():
                    wait_bytes(aside.at[a, owner_of(way, k)], h_recv.at[a, way, k - 1])
                    if k < n - 1:
                        @pl.when(reach(way, k))
                        def _():
                            aside_hop(a, way, k).start()
                    aside_out(a, way, k).start()
        for a in range(2):
            for way in range(2):
                for side, cols in variants:
                    @pl.when(both(side, arrives(way, k)))
                    def _():
                        wait_bytes(shard(a, owner_of(way, k), cols), w_recv.at[a, way, k - 1])

                    if k < n - 1:
                        @pl.when(both(side, reach(way, k)))
                        def _():
                            hop(a, way, k, cols).start()
        for a in range(2):
            for way in range(2):
                @pl.when(both(high, arrives(way, k)))
                def _():
                    wait_bytes(shard(a, owner_of(way, k), rest), o_recv.at[a, way, k])

                if early:
                    @pl.when(arrives(way, k))
                    def _():
                        turn(a, owner_of(way, k))
    if not early:
        for a in range(2):
            turned[a][...] = fulls[a][...].T

    gain_out[...] = jnp.zeros_like(gain_out)

    def pair_copy(i, b):
        rows = pl.ds(pl.multiple_of(b * rows_per, rows_per), rows_per)
        return pltpu.make_async_remote_copy(
            src_ref=tx.at[i, rows], dst_ref=rx.at[i, rows],
            send_sem=p_send.at[i], recv_sem=p_recv.at[i, b],
            device_id=(s - 1, d), device_id_type=MESH,
        )

    def take(i, b, rows, source, column):
        @pl.when(is_last)
        def _():
            held[i] = source[rows, column].astype(f32)

        @pl.when(not_last)
        def _():
            rows_ = pl.ds(pl.multiple_of(b * rows_per, rows_per), rows_per)
            pltpu.make_async_remote_copy(
                src_ref=tx.at[i, rows_], dst_ref=rx.at[i, rows_],
                send_sem=p_send.at[i], recv_sem=p_recv.at[i, b],
                device_id=(s + 1, d), device_id_type=MESH,
            ).wait_recv()
            held[i] = rx[i, rows].astype(f32)

    def give(i, b, rows, values):
        tx[i, rows] = values.astype(bf16)

        @pl.when(has_below)
        def _():
            pair_copy(i, b).start()

    def share_norm(a, rows, normed):
        for e in range(n):
            norms_own[a, e, rows] = normed[:, e * part:(e + 1) * part]
        for k in range(1, n):
            e = peer(k)
            pltpu.make_async_remote_copy(
                src_ref=norms_own.at[a, e, rows], dst_ref=norms.at[a, d, rows],
                send_sem=n_send.at[a], recv_sem=n_recv.at[a],
                device_id=(s, e), device_id_type=MESH,
            ).start()

    split = h - late.shape[2]
    tail = pl.ds(split, h - split)
    delta_variants = (
        ((jnp.bool_(True), pl.ds(0, h)),), ((low, pl.ds(0, split)), (high, pl.ds(0, h))),
    )

    def late_in(rows):
        return pltpu.make_async_remote_copy(
            src_ref=deltas.at[1, d, rows, tail], dst_ref=late.at[d, rows],
            send_sem=l_sem.at[0], recv_sem=l_sem.at[1],
            device_id=(partner, d), device_id_type=MESH,
        )

    def late_hop(way, k):
        owner = owner_of(way, k)
        return pltpu.make_async_remote_copy(
            src_ref=late.at[owner], dst_ref=late.at[owner],
            send_sem=lh_send.at[way, k], recv_sem=lh_recv.at[way, k],
            device_id=(s, ahead(way)), device_id_type=MESH,
        )

    def late_out(way, k):
        owner = owner_of(way, k)
        return pltpu.make_async_remote_copy(
            src_ref=late.at[owner], dst_ref=deltas.at[1, owner, pl.ds(0, tokens), tail],
            send_sem=lo_send.at[way, k], recv_sem=lo_recv.at[way, k],
            device_id=(partner, d), device_id_type=MESH,
        )

    def delta_hop(a, way, k, rows, cols):
        owner = d - k if way == 0 else d + k
        return pltpu.make_async_remote_copy(
            src_ref=deltas.at[a, owner, rows, cols], dst_ref=deltas.at[a, owner, rows, cols],
            send_sem=d_send.at[a, way, k], recv_sem=d_recv.at[a, way, k],
            device_id=(s, d + 1 if way == 0 else d - 1), device_id_type=MESH,
        )

    def share_delta(a, rows, delta):
        deltas[a, d, rows] = delta
        for way in range(2):
            for side, cols in delta_variants[a]:
                @pl.when(both(side, reach(way, 0)))
                def _():
                    delta_hop(a, way, 0, rows, cols).start()
        if a == 1:
            @pl.when(low)
            def _():
                late_in(rows).start()

    first, second = pl.ds(0, h), pl.ds(h, h)

    def block(b, carry):
        rows = pl.ds(pl.multiple_of(b * rows_per, rows_per), rows_per)
        gain_f, gain_g = gains_ref[0:1, :], gains_ref[1:2, :]
        take(0, b, rows, pair_ref, first)
        y1 = held[0]
        r1 = inverse_scale(y1)
        norm_g = (y1 * r1 * gain_g).astype(bf16)
        pre_g = jnp.dot(norm_g, wg[...], preferred_element_type=f32)
        take(1, b, rows, pair_ref, second)
        act_g, slope_g = silu_parts(pre_g)
        x2 = held[1] - act_g
        in_pair_ref[rows, second] = x2
        give(1, b, rows, x2)
        slopes[0] = slope_g
        r2 = inverse_scale(x2)
        norm_f = (x2 * r2 * gain_f).astype(bf16)
        pre_f = jnp.dot(norm_f, wf[...], preferred_element_type=f32)
        act_f, slope_f = silu_parts(pre_f)
        x1 = held[0] - act_f
        in_pair_ref[rows, first] = x1
        give(0, b, rows, x1)
        slopes[1] = slope_f
        share_norm(0, rows, norm_f)
        share_norm(1, rows, norm_g)

        take(3, b, rows, grad_ref, second)
        take(2, b, rows, grad_ref, first)
        delta_g = (held[3] * slopes[0]).astype(bf16)
        back_g = jnp.dot(delta_g, wgt[...], preferred_element_type=f32)
        share_delta(1, rows, delta_g)
        y1 = held[0]
        weighted = gain_g * back_g
        gz = held[2] + r1 * weighted - y1 * (r1 * r1 * r1) * jnp.mean(
            weighted * y1, axis=-1, keepdims=True
        )
        in_grad_ref[rows, first] = gz.astype(bf16)
        give(2, b, rows, gz)
        gain_out[1:2, :] += jnp.sum(back_g * y1 * r1, axis=0, keepdims=True)
        delta_f = (gz * slopes[1]).astype(bf16)
        back_f = jnp.dot(delta_f, wft[...], preferred_element_type=f32)
        share_delta(0, rows, delta_f)
        x2 = in_pair_ref[rows, second]
        weighted = gain_f * back_f
        gx2 = held[3] + r2 * weighted - x2 * (r2 * r2 * r2) * jnp.mean(
            weighted * x2, axis=-1, keepdims=True
        )
        in_grad_ref[rows, second] = gx2.astype(bf16)
        give(3, b, rows, gx2)
        gain_out[0:1, :] += jnp.sum(back_f * x2 * r2, axis=0, keepdims=True)
        return carry

    lax.fori_loop(0, blocks, block, 0)

    gain_parts[d] = gain_out[...]
    for k in range(1, n):
        pltpu.make_async_remote_copy(
            src_ref=gain_parts.at[d], dst_ref=gain_parts.at[d],
            send_sem=c_send, recv_sem=c_recv,
            device_id=(s, peer(k)), device_id_type=MESH,
        ).start()

    for a in range(2):
        norms[a, d] = norms_own[a, d]
    others, whole = pl.ds(0, n - 1), pl.ds(0, tokens)
    for k in range(1, n):
        for a in (1, 0):
            for way in range(2):
                for side, cols in delta_variants[a]:
                    @pl.when(both(side, arrives(way, k)))
                    def _():
                        wait_bytes(
                            deltas.at[a, owner_of(way, k), whole, cols], d_recv.at[a, way, k - 1]
                        )

                    if k < n - 1:
                        @pl.when(both(side, reach(way, k)))
                        def _():
                            delta_hop(a, way, k, whole, cols).start()
    for a, out in ((0, f_out), (1, g_out)):
        if a == 1:
            for k in range(1, n):
                for way in range(2):
                    @pl.when(both(low, arrives(way, k)))
                    def _():
                        wait_bytes(deltas.at[1, owner_of(way, k), whole, tail], lo_recv.at[way, k])
        wait_bytes(norms.at[a, others], n_recv.at[a])
        out[...] = lax.dot_general(
            norms[a].reshape(n * tokens, part), deltas[a].reshape(n * tokens, h),
            (((0,), (0,)), ((), ())), preferred_element_type=f32,
        )

    @pl.when(high)
    def _():
        wait_bytes(late.at[d], l_sem.at[1])
        for way in range(2):
            @pl.when(reach(way, 0))
            def _():
                late_hop(way, 0).start()
        for k in range(1, n):
            for way in range(2):
                @pl.when(arrives(way, k))
                def _():
                    wait_bytes(late.at[owner_of(way, k)], lh_recv.at[way, k - 1])
                    if k < n - 1:
                        @pl.when(reach(way, k))
                        def _():
                            late_hop(way, k).start()
                    late_out(way, k).start()
        for k in range(n):
            for way in range(2):
                if k < n - 1:
                    @pl.when(reach(way, k))
                    def _():
                        late_hop(way, k).wait_send()
                if k > 0:
                    @pl.when(arrives(way, k))
                    def _():
                        late_out(way, k).wait_send()

    @pl.when(low)
    def _():
        wait_bytes(late.at[d], l_sem.at[0])

    wait_bytes(gain_parts.at[others], c_recv)
    total = gain_parts[0]
    for e in range(1, n):
        total = total + gain_parts[e]
    gain_out[...] = total

    for a in range(2):
        wait_bytes(norms.at[a, others], n_send.at[a])
        for k in range(n - 1):
            for way in range(2):
                for side, cols in delta_variants[a]:
                    @pl.when(both(side, reach(way, k)))
                    def _():
                        wait_bytes(
                            deltas.at[a, owner_of(way, k), whole, cols], d_send.at[a, way, k]
                        )
    wait_bytes(gain_parts.at[others], c_send)

    @pl.when(has_below)
    def _():
        for i in range(4):
            wait_bytes(tx.at[i], p_send.at[i])

    @pl.when(high)
    def _():
        for a in range(2):
            aside_in(a).wait_send()

    for k in range(n):
        for a in range(2):
            for way in range(2):
                if k < n - 1:
                    for side, cols in variants:
                        @pl.when(both(side, reach(way, k)))
                        def _():
                            hop(a, way, k, cols).wait_send()

                    @pl.when(both(low, reach(way, k)))
                    def _():
                        aside_hop(a, way, k).wait_send()
                if k > 0:
                    @pl.when(both(low, arrives(way, k)))
                    def _():
                        aside_out(a, way, k).wait_send()


def shards(out_pair, out_grad, f_weight, g_weight, gains):
    n, sections = lax.axis_size("dp"), lax.axis_size("section")
    tokens, width = out_pair.shape
    h = width // 2
    part = f_weight.shape[1]
    blocks = 4
    vmem = pl.BlockSpec(memory_space=pltpu.VMEM)
    dma = pltpu.SemaphoreType.DMA
    outs = pl.pallas_call(
        functools.partial(kernel, n, sections, blocks),
        out_shape=(
            jax.ShapeDtypeStruct((tokens, width), f32),
            jax.ShapeDtypeStruct((tokens, width), bf16),
            jax.ShapeDtypeStruct((part, h), f32),
            jax.ShapeDtypeStruct((part, h), f32),
            jax.ShapeDtypeStruct((2, h), f32),
        ),
        in_specs=[vmem] * 5,
        out_specs=[vmem] * 5,
        scratch_shapes=[
            pltpu.VMEM((h, h), bf16),
            pltpu.VMEM((h, h), bf16),
            pltpu.VMEM((h, h), bf16),
            pltpu.VMEM((h, h), bf16),
            pltpu.VMEM((2, n, part, h // 8), bf16),
            pltpu.VMEM((n, tokens, h // 2), bf16),
            pltpu.VMEM((4, tokens, h), bf16),
            pltpu.VMEM((4, tokens, h), bf16),
            pltpu.VMEM((4, tokens // blocks, h), f32),
            pltpu.VMEM((2, tokens // blocks, h), f32),
            pltpu.VMEM((2, n, tokens, part), bf16),
            pltpu.VMEM((2, n, tokens, part), bf16),
            pltpu.VMEM((2, n, tokens, h), bf16),
            pltpu.VMEM((n, 2, h), f32),
            dma((2,)),
            dma((2, n)),
            dma((2, n)),
            dma((2, n)),
            dma((2, n)),
            dma((2,)),
            dma((2,)),
            dma((2,)),
            dma((2, 2, n)),
            dma((2, 2, n)),
            dma((2, 2, n)),
            dma((2, 2, n)),
            dma((2, 2, n)),
            dma((2, 2, n)),
            dma((4,)),
            dma((4, blocks)),
            dma((2,)),
            dma((2,)),
            dma((2, 2, n)),
            dma((2, 2, n)),
            dma,
            dma,
        ],
        compiler_params=pltpu.CompilerParams(
            collective_id=0, has_side_effects=True, vmem_limit_bytes=60 * 1024 * 1024
        ),
    )(out_pair, out_grad, f_weight[0], g_weight[0], gains[0])
    return tuple(out[None] for out in outs)


def solution(mesh):
    placed = (
        P("dp", None),
        P("dp", None),
        P("section", "dp", None),
        P("section", "dp", None),
        P("section", None, None),
    )
    return jax.shard_map(
        shards,
        mesh=mesh,
        in_specs=placed,
        out_specs=(
            P("section", "dp", None),
            P("section", "dp", None),
            P("section", "dp", None),
            P("section", "dp", None),
            P("section", None, None),
        ),
        check_vma=False,
    )
```

```python
import functools

import jax
import jax.numpy as jnp
from jax import lax
from jax.experimental import pallas as pl
from jax.experimental.pallas import tpu as pltpu
from jax.sharding import PartitionSpec as P

offset = 0.25
MESH = pl.DeviceIdType.MESH
f32, bf16 = jnp.float32, jnp.bfloat16


def silu_parts(pre_values):
    sigmoid_value = jax.nn.sigmoid(pre_values)
    return (pre_values * sigmoid_value, sigmoid_value * (1.0 + pre_values * (1.0 - sigmoid_value)))


def inverse_scale(values):
    return lax.rsqrt(jnp.mean(values * values, axis=-1, keepdims=True) + offset)


def kernel(
    n, sections, blocks,
    pair_ref, grad_ref, fw_ref, gw_ref, gains_ref,
    in_pair_ref, in_grad_ref, f_out, g_out, gain_out,
    wf, wg, wft, wgt, aside, late, rx, tx, held, slopes, norms_own, norms, deltas, gain_parts,
    l_sem, lh_send, lh_recv, lo_send, lo_recv, own_sem, i_send, i_recv, h_send, h_recv, o_send, o_recv, w_send, w_recv, p_send, p_recv, n_send, n_recv, d_send, d_recv, c_send, c_recv,
):
    s, d = lax.axis_index("section"), lax.axis_index("dp")
    is_last = s == sections - 1
    has_below = s > 0
    not_last = jnp.logical_not(is_last)
    tokens = pair_ref.shape[0]
    h = pair_ref.shape[1] // 2
    part = fw_ref.shape[0]
    rows_per = tokens // blocks

    def peer(k):
        return lax.rem(d + k, n)

    barrier = pltpu.get_barrier_semaphore()
    for k in range(1, n):
        pl.semaphore_signal(barrier, inc=1, device_id=(s, peer(k)), device_id_type=MESH)

    @pl.when(has_below)
    def _():
        pl.semaphore_signal(barrier, inc=1, device_id=(s - 1, d), device_id_type=MESH)

    @pl.when(not_last)
    def _():
        pl.semaphore_signal(barrier, inc=1, device_id=(s + 1, d), device_id_type=MESH)

    half = sections // 2
    partner = lax.rem(s + half, sections)
    high, low = s >= half, s < half
    pl.semaphore_signal(barrier, inc=1, device_id=(partner, d), device_id_type=MESH)
    neighbours = n + has_below.astype(jnp.int32) + not_last.astype(jnp.int32)
    pl.semaphore_wait(barrier, neighbours)

    fulls, owns, turned = (wg, wf), (gw_ref, fw_ref), (wgt, wft)
    keep = h - aside.shape[3]
    variants = ((low, pl.ds(0, h)), (high, pl.ds(0, keep)))
    rest = pl.ds(keep, h - keep)

    def shard(a, owner, cols):
        return fulls[a].at[pl.ds(pl.multiple_of(owner * part, part), part), cols]

    def owner_of(way, k):
        return d - k if way == 0 else d + k

    def ahead(way):
        return d + 1 if way == 0 else d - 1

    def hop(a, way, k, cols):
        owner = owner_of(way, k)
        src = owns[a].at[:, cols] if k == 0 else shard(a, owner, cols)
        return pltpu.make_async_remote_copy(
            src_ref=src, dst_ref=shard(a, owner, cols),
            send_sem=w_send.at[a, way, k], recv_sem=w_recv.at[a, way, k],
            device_id=(s, ahead(way)), device_id_type=MESH,
        )

    def aside_in(a):
        return pltpu.make_async_remote_copy(
            src_ref=owns[a].at[:, rest], dst_ref=aside.at[a, d],
            send_sem=i_send.at[a], recv_sem=i_recv.at[a],
            device_id=(partner, d), device_id_type=MESH,
        )

    def aside_hop(a, way, k):
        owner = owner_of(way, k)
        return pltpu.make_async_remote_copy(
            src_ref=aside.at[a, owner], dst_ref=aside.at[a, owner],
            send_sem=h_send.at[a, way, k], recv_sem=h_recv.at[a, way, k],
            device_id=(s, ahead(way)), device_id_type=MESH,
        )

    def aside_out(a, way, k):
        owner = owner_of(way, k)
        return pltpu.make_async_remote_copy(
            src_ref=aside.at[a, owner], dst_ref=shard(a, owner, rest),
            send_sem=o_send.at[a, way, k], recv_sem=o_recv.at[a, way, k],
            device_id=(partner, d), device_id_type=MESH,
        )

    def wait_bytes(ref, sem):
        pltpu.make_async_copy(ref, ref, sem).wait()

    def reach(way, k):
        if way == 0:
            return jnp.logical_and(d - k >= 0, d < n - 1)
        return jnp.logical_and(d + k < n, d > 0)

    def arrives(way, k):
        return d - k >= 0 if way == 0 else d + k < n

    both = jnp.logical_and

    @pl.when(high)
    def _():
        for a in range(2):
            aside_in(a).start()

    @pl.when(low)
    def _():
        for a in range(2):
            wait_bytes(aside.at[a, d], i_recv.at[a])
            for way in range(2):
                @pl.when(reach(way, 0))
                def _():
                    aside_hop(a, way, 0).start()

    for a in range(2):
        for way in range(2):
            for side, cols in variants:
                @pl.when(both(side, reach(way, 0)))
                def _():
                    hop(a, way, 0, cols).start()
    early = part % 128 == 0

    def turn(a, owner):
        span = pl.ds(pl.multiple_of(owner * part, part), part)
        turned[a][:, span] = fulls[a][span, :].T

    own_copies = [
        pltpu.make_async_copy(owns[a], shard(a, d, pl.ds(0, h)), own_sem.at[a]) for a in range(2)
    ]
    for copy in own_copies:
        copy.start()
    for a, copy in enumerate(own_copies):
        copy.wait()
        if early:
            turn(a, d)
    for k in range(1, n):
        for a in range(2):
            for way in range(2):
                @pl.when(both(low, arrives(way, k)))
                def _():
                    wait_bytes(aside.at[a, owner_of(way, k)], h_recv.at[a, way, k - 1])
                    if k < n - 1:
                        @pl.when(reach(way, k))
                        def _():
                            aside_hop(a, way, k).start()
                    aside_out(a, way, k).start()
        for a in range(2):
            for way in range(2):
                for side, cols in variants:
                    @pl.when(both(side, arrives(way, k)))
                    def _():
                        wait_bytes(shard(a, owner_of(way, k), cols), w_recv.at[a, way, k - 1])

                    if k < n - 1:
                        @pl.when(both(side, reach(way, k)))
                        def _():
                            hop(a, way, k, cols).start()
        for a in range(2):
            for way in range(2):
                @pl.when(both(high, arrives(way, k)))
                def _():
                    wait_bytes(shard(a, owner_of(way, k), rest), o_recv.at[a, way, k])

                if early:
                    @pl.when(arrives(way, k))
                    def _():
                        turn(a, owner_of(way, k))
    if not early:
        for a in range(2):
            turned[a][...] = fulls[a][...].T

    gain_out[...] = jnp.zeros_like(gain_out)

    def pair_copy(i, b):
        rows = pl.ds(pl.multiple_of(b * rows_per, rows_per), rows_per)
        return pltpu.make_async_remote_copy(
            src_ref=tx.at[i, rows], dst_ref=rx.at[i, rows],
            send_sem=p_send.at[i], recv_sem=p_recv.at[i, b],
            device_id=(s - 1, d), device_id_type=MESH,
        )

    def take(i, b, rows, source, column):
        @pl.when(is_last)
        def _():
            held[i] = source[rows, column].astype(f32)

        @pl.when(not_last)
        def _():
            rows_ = pl.ds(pl.multiple_of(b * rows_per, rows_per), rows_per)
            pltpu.make_async_remote_copy(
                src_ref=tx.at[i, rows_], dst_ref=rx.at[i, rows_],
                send_sem=p_send.at[i], recv_sem=p_recv.at[i, b],
                device_id=(s + 1, d), device_id_type=MESH,
            ).wait_recv()
            held[i] = rx[i, rows].astype(f32)

    def give(i, b, rows, values):
        tx[i, rows] = values.astype(bf16)

        @pl.when(has_below)
        def _():
            pair_copy(i, b).start()

    def share_norm(a, rows, normed):
        for e in range(n):
            norms_own[a, e, rows] = normed[:, e * part:(e + 1) * part]
        for k in range(1, n):
            e = peer(k)
            pltpu.make_async_remote_copy(
                src_ref=norms_own.at[a, e, rows], dst_ref=norms.at[a, d, rows],
                send_sem=n_send.at[a], recv_sem=n_recv.at[a],
                device_id=(s, e), device_id_type=MESH,
            ).start()

    split = h - late.shape[2]
    tail = pl.ds(split, h - split)
    delta_variants = (
        ((jnp.bool_(True), pl.ds(0, h)),), ((low, pl.ds(0, split)), (high, pl.ds(0, h))),
    )

    def late_in(rows):
        return pltpu.make_async_remote_copy(
            src_ref=deltas.at[1, d, rows, tail], dst_ref=late.at[d, rows],
            send_sem=l_sem.at[0], recv_sem=l_sem.at[1],
            device_id=(partner, d), device_id_type=MESH,
        )

    def late_hop(way, k):
        owner = owner_of(way, k)
        return pltpu.make_async_remote_copy(
            src_ref=late.at[owner], dst_ref=late.at[owner],
            send_sem=lh_send.at[way, k], recv_sem=lh_recv.at[way, k],
            device_id=(s, ahead(way)), device_id_type=MESH,
        )

    def late_out(way, k):
        owner = owner_of(way, k)
        return pltpu.make_async_remote_copy(
            src_ref=late.at[owner], dst_ref=deltas.at[1, owner, pl.ds(0, tokens), tail],
            send_sem=lo_send.at[way, k], recv_sem=lo_recv.at[way, k],
            device_id=(partner, d), device_id_type=MESH,
        )

    def delta_hop(a, way, k, rows, cols):
        owner = d - k if way == 0 else d + k
        return pltpu.make_async_remote_copy(
            src_ref=deltas.at[a, owner, rows, cols], dst_ref=deltas.at[a, owner, rows, cols],
            send_sem=d_send.at[a, way, k], recv_sem=d_recv.at[a, way, k],
            device_id=(s, d + 1 if way == 0 else d - 1), device_id_type=MESH,
        )

    def share_delta(a, rows, delta):
        deltas[a, d, rows] = delta
        for way in range(2):
            for side, cols in delta_variants[a]:
                @pl.when(both(side, reach(way, 0)))
                def _():
                    delta_hop(a, way, 0, rows, cols).start()
        if a == 1:
            @pl.when(low)
            def _():
                late_in(rows).start()

    first, second = pl.ds(0, h), pl.ds(h, h)

    def block(b, carry):
        rows = pl.ds(pl.multiple_of(b * rows_per, rows_per), rows_per)
        gain_f, gain_g = gains_ref[0:1, :], gains_ref[1:2, :]
        take(0, b, rows, pair_ref, first)
        y1 = held[0]
        r1 = inverse_scale(y1)
        norm_g = (y1 * r1 * gain_g).astype(bf16)
        pre_g = jnp.dot(norm_g, wg[...], preferred_element_type=f32)
        take(1, b, rows, pair_ref, second)
        act_g, slope_g = silu_parts(pre_g)
        x2 = held[1] - act_g
        in_pair_ref[rows, second] = x2
        give(1, b, rows, x2)
        slopes[0] = slope_g
        r2 = inverse_scale(x2)
        norm_f = (x2 * r2 * gain_f).astype(bf16)
        pre_f = jnp.dot(norm_f, wf[...], preferred_element_type=f32)
        act_f, slope_f = silu_parts(pre_f)
        x1 = held[0] - act_f
        in_pair_ref[rows, first] = x1
        give(0, b, rows, x1)
        slopes[1] = slope_f
        share_norm(0, rows, norm_f)
        share_norm(1, rows, norm_g)

        take(3, b, rows, grad_ref, second)
        take(2, b, rows, grad_ref, first)
        delta_g = (held[3] * slopes[0]).astype(bf16)
        back_g = jnp.dot(delta_g, wgt[...], preferred_element_type=f32)
        share_delta(1, rows, delta_g)
        y1 = held[0]
        weighted = gain_g * back_g
        gz = held[2] + r1 * weighted - y1 * (r1 * r1 * r1) * jnp.mean(
            weighted * y1, axis=-1, keepdims=True
        )
        in_grad_ref[rows, first] = gz.astype(bf16)
        give(2, b, rows, gz)
        gain_out[1:2, :] += jnp.sum(back_g * y1 * r1, axis=0, keepdims=True)
        delta_f = (gz * slopes[1]).astype(bf16)
        back_f = jnp.dot(delta_f, wft[...], preferred_element_type=f32)
        share_delta(0, rows, delta_f)
        x2 = in_pair_ref[rows, second]
        weighted = gain_f * back_f
        gx2 = held[3] + r2 * weighted - x2 * (r2 * r2 * r2) * jnp.mean(
            weighted * x2, axis=-1, keepdims=True
        )
        in_grad_ref[rows, second] = gx2.astype(bf16)
        give(3, b, rows, gx2)
        gain_out[0:1, :] += jnp.sum(back_f * x2 * r2, axis=0, keepdims=True)
        return carry

    lax.fori_loop(0, blocks, block, 0)

    gain_parts[d] = gain_out[...]
    for k in range(1, n):
        pltpu.make_async_remote_copy(
            src_ref=gain_parts.at[d], dst_ref=gain_parts.at[d],
            send_sem=c_send, recv_sem=c_recv,
            device_id=(s, peer(k)), device_id_type=MESH,
        ).start()

    for a in range(2):
        norms[a, d] = norms_own[a, d]
    others, whole = pl.ds(0, n - 1), pl.ds(0, tokens)
    for k in range(1, n):
        for a in (1, 0):
            for way in range(2):
                for side, cols in delta_variants[a]:
                    @pl.when(both(side, arrives(way, k)))
                    def _():
                        wait_bytes(
                            deltas.at[a, owner_of(way, k), whole, cols], d_recv.at[a, way, k - 1]
                        )

                    if k < n - 1:
                        @pl.when(both(side, reach(way, k)))
                        def _():
                            delta_hop(a, way, k, whole, cols).start()
    @pl.when(high)
    def _():
        wait_bytes(late.at[d], l_sem.at[1])
        for way in range(2):
            @pl.when(reach(way, 0))
            def _():
                late_hop(way, 0).start()

    for a, out in ((0, f_out), (1, g_out)):
        if a == 1:
            for k in range(1, n):
                for way in range(2):
                    @pl.when(both(low, arrives(way, k)))
                    def _():
                        wait_bytes(deltas.at[1, owner_of(way, k), whole, tail], lo_recv.at[way, k])
        wait_bytes(norms.at[a, others], n_recv.at[a])
        out[...] = lax.dot_general(
            norms[a].reshape(n * tokens, part), deltas[a].reshape(n * tokens, h),
            (((0,), (0,)), ((), ())), preferred_element_type=f32,
        )

    @pl.when(high)
    def _():
        for k in range(1, n):
            for way in range(2):
                @pl.when(arrives(way, k))
                def _():
                    wait_bytes(late.at[owner_of(way, k)], lh_recv.at[way, k - 1])
                    if k < n - 1:
                        @pl.when(reach(way, k))
                        def _():
                            late_hop(way, k).start()
                    late_out(way, k).start()
        for k in range(n):
            for way in range(2):
                if k < n - 1:
                    @pl.when(reach(way, k))
                    def _():
                        late_hop(way, k).wait_send()
                if k > 0:
                    @pl.when(arrives(way, k))
                    def _():
                        late_out(way, k).wait_send()

    @pl.when(low)
    def _():
        wait_bytes(late.at[d], l_sem.at[0])

    wait_bytes(gain_parts.at[others], c_recv)
    total = gain_parts[0]
    for e in range(1, n):
        total = total + gain_parts[e]
    gain_out[...] = total

    for a in range(2):
        wait_bytes(norms.at[a, others], n_send.at[a])
        for k in range(n - 1):
            for way in range(2):
                for side, cols in delta_variants[a]:
                    @pl.when(both(side, reach(way, k)))
                    def _():
                        wait_bytes(
                            deltas.at[a, owner_of(way, k), whole, cols], d_send.at[a, way, k]
                        )
    wait_bytes(gain_parts.at[others], c_send)

    @pl.when(has_below)
    def _():
        for i in range(4):
            wait_bytes(tx.at[i], p_send.at[i])

    @pl.when(high)
    def _():
        for a in range(2):
            aside_in(a).wait_send()

    for k in range(n):
        for a in range(2):
            for way in range(2):
                if k < n - 1:
                    for side, cols in variants:
                        @pl.when(both(side, reach(way, k)))
                        def _():
                            hop(a, way, k, cols).wait_send()

                    @pl.when(both(low, reach(way, k)))
                    def _():
                        aside_hop(a, way, k).wait_send()
                if k > 0:
                    @pl.when(both(low, arrives(way, k)))
                    def _():
                        aside_out(a, way, k).wait_send()


def shards(out_pair, out_grad, f_weight, g_weight, gains):
    n, sections = lax.axis_size("dp"), lax.axis_size("section")
    tokens, width = out_pair.shape
    h = width // 2
    part = f_weight.shape[1]
    blocks = 4
    vmem = pl.BlockSpec(memory_space=pltpu.VMEM)
    dma = pltpu.SemaphoreType.DMA
    outs = pl.pallas_call(
        functools.partial(kernel, n, sections, blocks),
        out_shape=(
            jax.ShapeDtypeStruct((tokens, width), f32),
            jax.ShapeDtypeStruct((tokens, width), bf16),
            jax.ShapeDtypeStruct((part, h), f32),
            jax.ShapeDtypeStruct((part, h), f32),
            jax.ShapeDtypeStruct((2, h), f32),
        ),
        in_specs=[vmem] * 5,
        out_specs=[vmem] * 5,
        scratch_shapes=[
            pltpu.VMEM((h, h), bf16),
            pltpu.VMEM((h, h), bf16),
            pltpu.VMEM((h, h), bf16),
            pltpu.VMEM((h, h), bf16),
            pltpu.VMEM((2, n, part, h // 8), bf16),
            pltpu.VMEM((n, tokens, h // 2), bf16),
            pltpu.VMEM((4, tokens, h), bf16),
            pltpu.VMEM((4, tokens, h), bf16),
            pltpu.VMEM((4, tokens // blocks, h), f32),
            pltpu.VMEM((2, tokens // blocks, h), f32),
            pltpu.VMEM((2, n, tokens, part), bf16),
            pltpu.VMEM((2, n, tokens, part), bf16),
            pltpu.VMEM((2, n, tokens, h), bf16),
            pltpu.VMEM((n, 2, h), f32),
            dma((2,)),
            dma((2, n)),
            dma((2, n)),
            dma((2, n)),
            dma((2, n)),
            dma((2,)),
            dma((2,)),
            dma((2,)),
            dma((2, 2, n)),
            dma((2, 2, n)),
            dma((2, 2, n)),
            dma((2, 2, n)),
            dma((2, 2, n)),
            dma((2, 2, n)),
            dma((4,)),
            dma((4, blocks)),
            dma((2,)),
            dma((2,)),
            dma((2, 2, n)),
            dma((2, 2, n)),
            dma,
            dma,
        ],
        compiler_params=pltpu.CompilerParams(
            collective_id=0, has_side_effects=True, vmem_limit_bytes=60 * 1024 * 1024
        ),
    )(out_pair, out_grad, f_weight[0], g_weight[0], gains[0])
    return tuple(out[None] for out in outs)


def solution(mesh):
    placed = (
        P("dp", None),
        P("dp", None),
        P("section", "dp", None),
        P("section", "dp", None),
        P("section", None, None),
    )
    return jax.shard_map(
        shards,
        mesh=mesh,
        in_specs=placed,
        out_specs=(
            P("section", "dp", None),
            P("section", "dp", None),
            P("section", "dp", None),
            P("section", "dp", None),
            P("section", None, None),
        ),
        check_vma=False,
    )
```
